32 devices in a mesh: rows: 8 (over z, y), dp: 4 (over x, core).
Axes of the slice: x: 2, y: 2, z: 4, core: 2. Of those that a mesh axis runs over, the one named last changes fastest.
Arguments:
- weights: float32 [6144, 4096], P(('rows', 'dp'))
- moment: float32 [6144, 4096], P(('rows', 'dp'))
- second: float32 [6144, 4096], P(('rows', 'dp')), may hold values from 0.01 to 1
- tile_rows: bfloat16 [2048, 4096], P(('rows', 'dp')), may hold values from -6 to 6
- row_index: int32 [2048], P(('rows', 'dp')), may hold values from 0 to 191
- bucket_count: int32 [1024], P(('rows', 'dp')), may hold values from 1 to 2, as said below
Outputs:
- new_weights: float32 [6144, 4096], P(('rows', 'dp'))
- new_moment: float32 [6144, 4096], P(('rows', 'dp'))
- new_second: float32 [6144, 4096], P(('rows', 'dp'))
The draws below stay inside these ranges and needn't reach their ends.
Inputs may be any that keep to these rules, and one draw needn't show every extreme that they name: `bucket_count`: at least one slot of every sender and owner is live; in every draw some owner receives 2 live slots from every sender. `row_index`: rows may repeat within and across senders.
All inputs are finite; a program needn't handle non-finite values.
Results may differ from the reference program's by a relative error of at most 0.0003.
Values may be sent and summed in bfloat16 or wider, within the bound.
A program may use at most 64 MiB of HBM per device.

```python
import math
import jax
import jax.numpy as jnp

D = 4096
ROWS_DEV = 192
CAP = 2
OWNERS = 32
VOCAB = 6144
SLOTS = 64


def draw_weights(key, part):
    key_one = jax.random.fold_in(key, 21)
    key_two = jax.random.fold_in(key, 22)
    key_three = jax.random.fold_in(key, 23)
    row_pos = jnp.arange(VOCAB, dtype=jnp.float32) / VOCAB
    normal_part = jax.random.truncated_normal(key_one, -4.0, 4.0, (VOCAB, D), jnp.float32)
    row_scale = 10.0 ** jax.random.uniform(key_two, (VOCAB, 1), jnp.float32) * 3.0 ** row_pos[:, None]
    col_scale = 10.0 ** jax.random.uniform(key_three, (1, D), jnp.float32)
    return 0.05 * normal_part * row_scale * col_scale


def draw_moment(key, part):
    key_one = jax.random.fold_in(key, 31)
    key_two = jax.random.fold_in(key, 32)
    row_pos = jnp.arange(VOCAB, dtype=jnp.float32) / VOCAB
    normal_part = jax.random.truncated_normal(key_one, -4.0, 4.0, (VOCAB, D), jnp.float32)
    row_scale = 10.0 ** jax.random.uniform(key_two, (VOCAB, 1), jnp.float32) * 3.0 ** row_pos[:, None]
    return 0.05 * normal_part * row_scale


def draw_bucket_count(key, part):
    key_one = jax.random.fold_in(key, 11)
    key_two = jax.random.fold_in(key, 12)
    counts_all = jax.random.randint(key_one, (OWNERS, OWNERS), 1, CAP + 1)
    full_owner = jax.random.randint(key_two, (), 0, OWNERS)
    column_id = jnp.arange(OWNERS)[None, :]
    return jnp.where(column_id == full_owner, CAP, counts_all).reshape(-1).astype(jnp.int32)


def touch_ends(entries, stream_key, least, largest):
    spot = [jax.random.randint(jax.random.fold_in(stream_key, axis), (), 0, length) for axis, length in enumerate(entries.shape)]
    widest = entries.shape.index(max(entries.shape))
    next_to = spot[:widest] + [(spot[widest] + 1) % entries.shape[widest]] + spot[widest + 1:]
    return entries.at[tuple(spot)].set(least).at[tuple(next_to)].set(largest)


def steps_of(stream_key, extent, split, least, largest):
    factor_of = 1.0
    for dim, shards_of in split:
        steps = jax.random.uniform(jax.random.fold_in(jax.random.fold_in(stream_key, 6), dim), (shards_of,), jnp.float32, least / len(split), largest / len(split))
        factor_of = factor_of * jnp.repeat(jnp.exp(steps), extent[dim] // shards_of).reshape((-1,) + (1,) * (len(extent) - 1 - dim))
    return factor_of


def gaussian(stream_key, extent, scale, limit, shards=(), kind=jnp.bfloat16):
    loudness = steps_of(stream_key, extent, shards, -0.22, 0.18) if shards else 1.0
    array = jax.random.normal(stream_key, extent, jnp.float32) * scale * loudness
    return jnp.minimum(jnp.maximum(array, -limit), limit).astype(kind)


def setup_inputs(seed: int = 0) -> dict:
    streams_of = jax.random.split(jax.random.key(seed), 7)
    return {
        "weights": draw_weights(jax.random.fold_in(streams_of[6], 71), 0),
        "moment": draw_moment(jax.random.fold_in(streams_of[6], 71), 0),
        "second": jnp.clip(jnp.exp(math.log(1.0) - 4.6051702 * jax.random.uniform(streams_of[2], (VOCAB, D), jnp.float32) ** steps_of(streams_of[2], (VOCAB, D), ((0, 32),), -0.2, 0.2)), 0.01, 1.0),
        "tile_rows": gaussian(streams_of[3], (OWNERS * SLOTS, D), 1.0, 6.0, ((0, 32),)),
        "row_index": touch_ends(jax.random.randint(streams_of[4], (OWNERS * SLOTS,), 0, ROWS_DEV), jax.random.fold_in(streams_of[4], 1), 0, ROWS_DEV - 1).astype(jnp.int32),
        "bucket_count": draw_bucket_count(jax.random.fold_in(streams_of[6], 71), 0),
    }


beta_one = 0.9
beta_two = 0.999
epsilon = 1e-06
decay = 0.01
rate = 0.1

def reference(weights, moment, second, tile_rows, row_index, bucket_count):
    position = jnp.arange(OWNERS * SLOTS, dtype=jnp.int32)
    slot_pos = position % CAP
    bucket_id = position // CAP
    owner_id = bucket_id % OWNERS
    is_live = slot_pos < bucket_count[bucket_id]
    table_row = jnp.where(is_live, owner_id * ROWS_DEV + row_index, 0).astype(jnp.int32)
    values = tile_rows.astype(jnp.float32) * is_live.astype(jnp.float32)[:, None]
    gradient = jax.ops.segment_sum(values, table_row, num_segments=VOCAB)
    new_moment = beta_one * moment + (1.0 - beta_one) * gradient
    new_second = beta_two * second + (1.0 - beta_two) * gradient * gradient
    update = new_moment / (jnp.sqrt(new_second) + epsilon) + decay * weights
    weight_sq = jnp.sum(weights * weights)
    update_sq = jnp.sum(update * update)
    trust_ratio = jnp.sqrt(weight_sq) / jnp.sqrt(update_sq + 1e-06)
    new_weights = weights - rate * trust_ratio * update
    return (new_weights, new_moment, new_second)
```

```python
import functools

import jax
import jax.numpy as jnp
from jax import lax
from jax.experimental import pallas as pl
from jax.experimental.pallas import tpu as pltpu
from jax.sharding import PartitionSpec as P

beta_one = 0.9
beta_two = 0.999
epsilon = 1e-06
decay = 0.01
rate = 0.1

AXES = ("rows", "dp")
LANES = 128
CHUNKS = 4


def exchange(
    n, fast, weights, moment, second, tiles, index, count,
    weight_out, moment_out, second_out, update_out, scale_out,
    staged, landed, index_all, count_all, parts, picker,
    load_sem, stage_sem, own_sem, tile_send, tile_recv, small_send, small_recv, part_send, part_recv,
):
    me = lax.axis_index("rows") * fast + lax.axis_index("dp")
    rows_here, width = weights.shape
    groups = width // LANES
    slots = index.shape[-1]
    capacity = slots // n
    per = groups // CHUNKS
    pack = tiles.shape[2]

    loads = [
        pltpu.make_async_copy(weights, weight_out, load_sem.at[0]),
        pltpu.make_async_copy(moment, moment_out, load_sem.at[1]),
        pltpu.make_async_copy(second, second_out, load_sem.at[2]),
    ]
    barrier = pltpu.get_barrier_semaphore()

    def place(device):
        return {"rows": device // fast, "dp": lax.rem(device, fast)}

    def peer_of(step):
        return lax.rem(me + 1 + lax.rem(step + n // 2 - 1, n - 1), n)

    @pl.loop(0, n - 1)
    def _(step):
        pl.semaphore_signal(
            barrier, inc=1, device_id=place(peer_of(step)),
            device_id_type=pl.DeviceIdType.MESH,
        )

    stage = [
        pltpu.make_async_copy(tiles, staged, stage_sem.at[0]),
        pltpu.make_async_copy(index, index_all.at[me], stage_sem.at[1]),
        pltpu.make_async_copy(count, count_all.at[me], stage_sem.at[2]),
    ]
    for copy in stage:
        copy.start()
    own = pltpu.make_async_copy(
        tiles.at[me // pack, :, lax.rem(me, pack)], landed.at[:, me], own_sem
    )
    own.start()
    for load in loads:
        load.start()
    for copy in stage:
        copy.wait()
    pl.semaphore_wait(barrier, n - 1)

    @pl.loop(0, n - 1)
    def _(step):
        peer = peer_of(step)
        for ref, k in ((index_all, 0), (count_all, 1)):
            pltpu.make_async_remote_copy(
                src_ref=ref.at[me], dst_ref=ref.at[me],
                send_sem=small_send.at[k], recv_sem=small_recv.at[k],
                device_id=place(peer), device_id_type=pl.DeviceIdType.MESH,
            ).start()

    for q in range(CHUNKS):
        span = pl.ds(q * per, per)

        @pl.loop(0, n - 1)
        def _(step):
            peer = peer_of(step)
            pltpu.make_async_remote_copy(
                src_ref=staged.at[peer // pack, span, lax.rem(peer, pack)],
                dst_ref=landed.at[span, me],
                send_sem=tile_send.at[q], recv_sem=tile_recv.at[q],
                device_id=place(peer), device_id_type=pl.DeviceIdType.MESH,
            ).start()

    loads[0].wait()

    def weight_step(g, total):
        w = weight_out[:, pl.ds(pl.multiple_of(g * LANES, LANES), LANES)]
        return total + jnp.sum((w * w).reshape(rows_here // 8, 8, LANES), axis=0)

    zero = jnp.zeros((8, LANES), jnp.float32)
    weight_sum = lax.fori_loop(0, groups, weight_step, zero, unroll=4)

    few = pl.ds(0, n - 1)
    for k, ref in enumerate((index_all, count_all)):
        pltpu.make_async_copy(ref.at[few], ref.at[few], small_recv.at[k]).wait()
    index_rows = index_all[:, 0, :]
    count_rows = count_all[:, 0, :]
    lane = lax.broadcasted_iota(jnp.int32, (n, slots), 1)
    sender = lax.broadcasted_iota(jnp.int32, (n, slots), 0)
    owner = lax.broadcasted_iota(jnp.int32, (n, n), 1)
    live = jnp.sum(jnp.where(owner == me, count_rows, 0), axis=1, keepdims=True)
    spread = jnp.zeros((n, slots), jnp.int32)
    for c in range(capacity):
        mine = jnp.sum(
            jnp.where(lane == me * capacity + c, index_rows, 0), axis=1, keepdims=True
        )
        mine = jnp.where(live > c, mine, -1)
        spread = spread + jnp.where(lane == sender * capacity + c, mine, 0)
    target = jnp.sum(spread, axis=0, keepdims=True)
    row = lax.broadcasted_iota(jnp.int32, (rows_here, slots), 0)
    picker[...] = jnp.where(row == target, 1.0, 0.0).astype(jnp.bfloat16)

    loads[1].wait()
    loads[2].wait()
    own.wait()
    update_sum = zero
    for q in range(CHUNKS):
        span = pl.ds(q * per, per)
        piece = landed.at[span, few]
        pltpu.make_async_copy(piece, piece, tile_recv.at[q]).wait()

        def step(g, total):
            cols = pl.ds(pl.multiple_of(g * LANES, LANES), LANES)
            block = landed[g].reshape(slots, LANES)
            gradient = jnp.dot(
                picker[...], block, preferred_element_type=jnp.float32
            )
            new_moment = beta_one * moment_out[:, cols] + (1.0 - beta_one) * gradient
            new_second = (
                beta_two * second_out[:, cols] + (1.0 - beta_two) * gradient * gradient
            )
            update = (
                new_moment / (jnp.sqrt(new_second) + epsilon)
                + decay * weight_out[:, cols]
            )
            moment_out[:, cols] = new_moment
            second_out[:, cols] = new_second
            update_out[:, cols] = update
            return total + jnp.sum(
                (update * update).reshape(rows_here // 8, 8, LANES), axis=0
            )

        update_sum = lax.fori_loop(q * per, (q + 1) * per, step, update_sum, unroll=4)

    parts[me, 0:1, :] = jnp.sum(weight_sum, axis=0, keepdims=True)
    parts[me, 1:2, :] = jnp.sum(update_sum, axis=0, keepdims=True)

    @pl.loop(0, n - 1)
    def _(step):
        pltpu.make_async_remote_copy(
            src_ref=parts.at[me], dst_ref=parts.at[me],
            send_sem=part_send, recv_sem=part_recv,
            device_id=place(peer_of(step)), device_id_type=pl.DeviceIdType.MESH,
        ).start()

    for k, ref in enumerate((index_all, count_all)):
        pltpu.make_async_copy(ref.at[few], ref.at[few], small_send.at[k]).wait()
    for q in range(CHUNKS):
        piece = landed.at[pl.ds(q * per, per), few]
        pltpu.make_async_copy(piece, piece, tile_send.at[q]).wait()
    pltpu.make_async_copy(parts.at[few], parts.at[few], part_recv).wait()
    pltpu.make_async_copy(parts.at[few], parts.at[few], part_send).wait()

    def total(k):
        lanes = jnp.sum(parts[:, k, :], axis=0, keepdims=True)
        return jnp.sum(lanes, axis=1, keepdims=True)

    trust = jnp.sqrt(total(0)) / jnp.sqrt(total(1) + 1e-06)
    scale_out[...] = jnp.broadcast_to(rate * trust, scale_out.shape)


def finish(
    weight, moment, second, update, scale,
    weight_out, moment_out, second_out, fresh, sem, piece_sem,
):
    copies = [
        pltpu.make_async_copy(moment, moment_out, sem.at[0]),
        pltpu.make_async_copy(second, second_out, sem.at[1]),
    ]
    for copy in copies:
        copy.start()
    rows_here = weight.shape[0]
    pieces = piece_sem.shape[0]
    height = rows_here // pieces
    factor = scale[0:1, 0:1]
    out = []
    for p in range(pieces):
        span = pl.ds(p * height, height)
        fresh[span, :] = weight[span, :] - factor * update[span, :]
        copy = pltpu.make_async_copy(
            fresh.at[span], weight_out.at[span], piece_sem.at[p]
        )
        copy.start()
        out.append(copy)
    for copy in copies + out:
        copy.wait()


def local(n, fast, weights, moment, second, tile_rows, row_index, bucket_count):
    rows_here, width = weights.shape
    slots = row_index.shape[0]
    capacity = slots // n
    groups = width // LANES
    pack = 8 // capacity
    tiles = tile_rows.reshape(n // pack, pack, capacity, groups, LANES)
    tiles = tiles.transpose(0, 3, 1, 2, 4)
    table = (rows_here, width)
    anywhere = pl.BlockSpec(memory_space=pl.ANY)
    outside = pl.BlockSpec(memory_space=pltpu.HBM)
    inside = pl.BlockSpec(memory_space=pltpu.VMEM)
    f32 = jnp.float32
    held = pltpu.VMEM(table, f32)
    weight_v, moment_v, second_v, update_v, scale = pl.pallas_call(
        functools.partial(exchange, n, fast),
        out_shape=[jax.ShapeDtypeStruct(table, f32)] * 4
        + [jax.ShapeDtypeStruct((8, LANES), f32)],
        in_specs=[outside] * 6,
        out_specs=[inside] * 5,
        scratch_shapes=[
            pltpu.VMEM(tiles.shape, jnp.bfloat16),
            pltpu.VMEM((groups, n, capacity, LANES), jnp.bfloat16),
            pltpu.VMEM((n, 1, slots), jnp.int32),
            pltpu.VMEM((n, 1, n), jnp.int32),
            pltpu.VMEM((n, 2, LANES), f32),
            pltpu.VMEM((rows_here, slots), jnp.bfloat16),
            pltpu.SemaphoreType.DMA((3,)),
            pltpu.SemaphoreType.DMA((3,)),
            pltpu.SemaphoreType.DMA,
            pltpu.SemaphoreType.DMA((CHUNKS,)),
            pltpu.SemaphoreType.DMA((CHUNKS,)),
            pltpu.SemaphoreType.DMA((2,)),
            pltpu.SemaphoreType.DMA((2,)),
            pltpu.SemaphoreType.DMA,
            pltpu.SemaphoreType.DMA,
        ],
        compiler_params=pltpu.CompilerParams(
            collective_id=0, has_side_effects=True, vmem_limit_bytes=24 * 1024 * 1024
        ),
        name="exchange",
    )(*(
        pltpu.with_memory_space_constraint(x, pltpu.HBM)
        for x in (
            weights, moment, second, tiles,
            row_index.reshape(1, slots), bucket_count.reshape(1, n),
        )
    ))
    pieces = 6
    return tuple(pl.pallas_call(
        finish,
        out_shape=[jax.ShapeDtypeStruct(table, f32)] * 3,
        in_specs=[inside] * 5,
        out_specs=[anywhere] * 3,
        scratch_shapes=[
            held,
            pltpu.SemaphoreType.DMA((2,)),
            pltpu.SemaphoreType.DMA((pieces,)),
        ],
        compiler_params=pltpu.CompilerParams(vmem_limit_bytes=24 * 1024 * 1024),
        name="finish",
    )(weight_v, moment_v, second_v, update_v, scale))


def solution(mesh):
    n = mesh.shape["rows"] * mesh.shape["dp"]
    rows, flat = P(AXES, None), P(AXES)
    return jax.shard_map(
        functools.partial(local, n, mesh.shape["dp"]),
        mesh=mesh,
        in_specs=(rows, rows, rows, rows, flat, flat),
        out_specs=(rows, rows, rows),
        check_vma=False,
    )
```

```python
import functools

import jax
import jax.numpy as jnp
from jax import lax
from jax.experimental import pallas as pl
from jax.experimental.pallas import tpu as pltpu
from jax.sharding import PartitionSpec as P

beta_one = 0.9
beta_two = 0.999
epsilon = 1e-06
decay = 0.01
rate = 0.1

AXES = ("rows", "dp")
LANES = 128
CHUNKS = 8


def exchange(
    n, fast, weights, moment, second, tiles, index, count,
    weight_out, moment_out, second_out, update_out, scale_out,
    staged, landed, index_all, count_all, parts, picker,
    load_sem, stage_sem, own_sem, tile_send, tile_recv, small_send, small_recv, part_send, part_recv,
):
    me = lax.axis_index("rows") * fast + lax.axis_index("dp")
    rows_here, width = weights.shape
    groups = width // LANES
    slots = index.shape[-1]
    capacity = slots // n
    per = groups // CHUNKS
    pack = tiles.shape[2]

    loads = [
        pltpu.make_async_copy(weights, weight_out, load_sem.at[0]),
        pltpu.make_async_copy(moment, moment_out, load_sem.at[1]),
        pltpu.make_async_copy(second, second_out, load_sem.at[2]),
    ]
    barrier = pltpu.get_barrier_semaphore()

    def place(device):
        return {"rows": device // fast, "dp": lax.rem(device, fast)}

    def peer_of(step):
        return lax.rem(me + 1 + step, n)

    @pl.loop(0, n - 1)
    def _(step):
        pl.semaphore_signal(
            barrier, inc=1, device_id=place(peer_of(step)),
            device_id_type=pl.DeviceIdType.MESH,
        )

    stage = [
        pltpu.make_async_copy(tiles, staged, stage_sem.at[0]),
        pltpu.make_async_copy(index, index_all.at[me], stage_sem.at[1]),
        pltpu.make_async_copy(count, count_all.at[me], stage_sem.at[2]),
    ]
    for copy in stage:
        copy.start()
    own = pltpu.make_async_copy(
        tiles.at[me // pack, :, lax.rem(me, pack)], landed.at[:, me], own_sem
    )
    own.start()
    for load in loads:
        load.start()
    for copy in stage:
        copy.wait()
    pl.semaphore_wait(barrier, n - 1)

    for q in range(CHUNKS):
        span = pl.ds(q * per, per)

        @pl.loop(0, n - 1)
        def _(step):
            peer = peer_of(step)
            pltpu.make_async_remote_copy(
                src_ref=staged.at[peer // pack, span, lax.rem(peer, pack)],
                dst_ref=landed.at[span, me],
                send_sem=tile_send.at[q], recv_sem=tile_recv.at[q],
                device_id=place(peer), device_id_type=pl.DeviceIdType.MESH,
            ).start()

        if q == 0:

            @pl.loop(0, n - 1)
            def _(step):
                peer = peer_of(step)
                for ref, k in ((index_all, 0), (count_all, 1)):
                    pltpu.make_async_remote_copy(
                        src_ref=ref.at[me], dst_ref=ref.at[me],
                        send_sem=small_send.at[k], recv_sem=small_recv.at[k],
                        device_id=place(peer), device_id_type=pl.DeviceIdType.MESH,
                    ).start()

    loads[0].wait()

    def weight_step(g, total):
        w = weight_out[:, pl.ds(pl.multiple_of(g * LANES, LANES), LANES)]
        return total + jnp.sum((w * w).reshape(rows_here // 8, 8, LANES), axis=0)

    zero = jnp.zeros((8, LANES), jnp.float32)
    weight_sum = lax.fori_loop(0, groups, weight_step, zero, unroll=4)

    few = pl.ds(0, n - 1)
    for k, ref in enumerate((index_all, count_all)):
        pltpu.make_async_copy(ref.at[few], ref.at[few], small_recv.at[k]).wait()
    index_rows = index_all[:, 0, :]
    count_rows = count_all[:, 0, :]
    lane = lax.broadcasted_iota(jnp.int32, (n, slots), 1)
    sender = lax.broadcasted_iota(jnp.int32, (n, slots), 0)
    owner = lax.broadcasted_iota(jnp.int32, (n, n), 1)
    live = jnp.sum(jnp.where(owner == me, count_rows, 0), axis=1, keepdims=True)
    spread = jnp.zeros((n, slots), jnp.int32)
    for c in range(capacity):
        mine = jnp.sum(
            jnp.where(lane == me * capacity + c, index_rows, 0), axis=1, keepdims=True
        )
        mine = jnp.where(live > c, mine, -1)
        spread = spread + jnp.where(lane == sender * capacity + c, mine, 0)
    target = jnp.sum(spread, axis=0, keepdims=True)
    row = lax.broadcasted_iota(jnp.int32, (rows_here, slots), 0)
    picker[...] = jnp.where(row == target, 1.0, 0.0).astype(jnp.bfloat16)

    loads[1].wait()
    loads[2].wait()
    own.wait()
    update_sum = zero
    for q in range(CHUNKS):
        span = pl.ds(q * per, per)
        piece = landed.at[span, few]
        pltpu.make_async_copy(piece, piece, tile_recv.at[q]).wait()

        def step(g, total):
            cols = pl.ds(pl.multiple_of(g * LANES, LANES), LANES)
            block = landed[g].reshape(slots, LANES)
            gradient = jnp.dot(
                picker[...], block, preferred_element_type=jnp.float32
            )
            new_moment = beta_one * moment_out[:, cols] + (1.0 - beta_one) * gradient
            new_second = (
                beta_two * second_out[:, cols] + (1.0 - beta_two) * gradient * gradient
            )
            update = (
                new_moment / (jnp.sqrt(new_second) + epsilon)
                + decay * weight_out[:, cols]
            )
            moment_out[:, cols] = new_moment
            second_out[:, cols] = new_second
            update_out[:, cols] = update
            return total + jnp.sum(
                (update * update).reshape(rows_here // 8, 8, LANES), axis=0
            )

        update_sum = lax.fori_loop(q * per, (q + 1) * per, step, update_sum, unroll=4)

    parts[me, 0:1, :] = jnp.sum(weight_sum, axis=0, keepdims=True)
    parts[me, 1:2, :] = jnp.sum(update_sum, axis=0, keepdims=True)

    @pl.loop(0, n - 1)
    def _(step):
        pltpu.make_async_remote_copy(
            src_ref=parts.at[me], dst_ref=parts.at[me],
            send_sem=part_send, recv_sem=part_recv,
            device_id=place(peer_of(step)), device_id_type=pl.DeviceIdType.MESH,
        ).start()

    for k, ref in enumerate((index_all, count_all)):
        pltpu.make_async_copy(ref.at[few], ref.at[few], small_send.at[k]).wait()
    for q in range(CHUNKS):
        piece = landed.at[pl.ds(q * per, per), few]
        pltpu.make_async_copy(piece, piece, tile_send.at[q]).wait()
    pltpu.make_async_copy(parts.at[few], parts.at[few], part_recv).wait()
    pltpu.make_async_copy(parts.at[few], parts.at[few], part_send).wait()

    def total(k):
        lanes = jnp.sum(parts[:, k, :], axis=0, keepdims=True)
        return jnp.sum(lanes, axis=1, keepdims=True)

    trust = jnp.sqrt(total(0)) / jnp.sqrt(total(1) + 1e-06)
    scale_out[...] = jnp.broadcast_to(rate * trust, scale_out.shape)


def finish(
    weight, moment, second, update, scale,
    weight_out, moment_out, second_out, fresh, sem, piece_sem,
):
    copies = [
        pltpu.make_async_copy(moment, moment_out, sem.at[0]),
        pltpu.make_async_copy(second, second_out, sem.at[1]),
    ]
    for copy in copies:
        copy.start()
    rows_here = weight.shape[0]
    pieces = piece_sem.shape[0]
    height = rows_here // pieces
    factor = scale[0:1, 0:1]
    out = []
    for p in range(pieces):
        span = pl.ds(p * height, height)
        fresh[span, :] = weight[span, :] - factor * update[span, :]
        copy = pltpu.make_async_copy(
            fresh.at[span], weight_out.at[span], piece_sem.at[p]
        )
        copy.start()
        out.append(copy)
    for copy in copies + out:
        copy.wait()


def local(n, fast, weights, moment, second, tile_rows, row_index, bucket_count):
    rows_here, width = weights.shape
    slots = row_index.shape[0]
    capacity = slots // n
    groups = width // LANES
    pack = 8 // capacity
    tiles = tile_rows.reshape(n // pack, pack, capacity, groups, LANES)
    tiles = tiles.transpose(0, 3, 1, 2, 4)
    table = (rows_here, width)
    anywhere = pl.BlockSpec(memory_space=pl.ANY)
    outside = pl.BlockSpec(memory_space=pltpu.HBM)
    inside = pl.BlockSpec(memory_space=pltpu.VMEM)
    f32 = jnp.float32
    held = pltpu.VMEM(table, f32)
    weight_v, moment_v, second_v, update_v, scale = pl.pallas_call(
        functools.partial(exchange, n, fast),
        out_shape=[jax.ShapeDtypeStruct(table, f32)] * 4
        + [jax.ShapeDtypeStruct((8, LANES), f32)],
        in_specs=[outside] * 6,
        out_specs=[inside] * 5,
        scratch_shapes=[
            pltpu.VMEM(tiles.shape, jnp.bfloat16),
            pltpu.VMEM((groups, n, capacity, LANES), jnp.bfloat16),
            pltpu.VMEM((n, 1, slots), jnp.int32),
            pltpu.VMEM((n, 1, n), jnp.int32),
            pltpu.VMEM((n, 2, LANES), f32),
            pltpu.VMEM((rows_here, slots), jnp.bfloat16),
            pltpu.SemaphoreType.DMA((3,)),
            pltpu.SemaphoreType.DMA((3,)),
            pltpu.SemaphoreType.DMA,
            pltpu.SemaphoreType.DMA((CHUNKS,)),
            pltpu.SemaphoreType.DMA((CHUNKS,)),
            pltpu.SemaphoreType.DMA((2,)),
            pltpu.SemaphoreType.DMA((2,)),
            pltpu.SemaphoreType.DMA,
            pltpu.SemaphoreType.DMA,
        ],
        compiler_params=pltpu.CompilerParams(
            collective_id=0, has_side_effects=True, vmem_limit_bytes=24 * 1024 * 1024
        ),
        name="exchange",
    )(*(
        pltpu.with_memory_space_constraint(x, pltpu.HBM)
        for x in (
            weights, moment, second, tiles,
            row_index.reshape(1, slots), bucket_count.reshape(1, n),
        )
    ))
    pieces = 6
    return tuple(pl.pallas_call(
        finish,
        out_shape=[jax.ShapeDtypeStruct(table, f32)] * 3,
        in_specs=[inside] * 5,
        out_specs=[anywhere] * 3,
        scratch_shapes=[
            held,
            pltpu.SemaphoreType.DMA((2,)),
            pltpu.SemaphoreType.DMA((pieces,)),
        ],
        compiler_params=pltpu.CompilerParams(vmem_limit_bytes=24 * 1024 * 1024),
        name="finish",
    )(weight_v, moment_v, second_v, update_v, scale))


def solution(mesh):
    n = mesh.shape["rows"] * mesh.shape["dp"]
    rows, flat = P(AXES, None), P(AXES)
    return jax.shard_map(
        functools.partial(local, n, mesh.shape["dp"]),
        mesh=mesh,
        in_specs=(rows, rows, rows, rows, flat, flat),
        out_specs=(rows, rows, rows),
        check_vma=False,
    )
```
